32 devices in a mesh: rows: 4 (over y, x), feat: 8 (over z, core).
Axes of the slice: x: 2, y: 2, z: 4, core: 2. Of those that a mesh axis runs over, the one named last changes fastest.
Arguments:
- bins: int32 [256, 32768], P(None, ('rows', 'feat')), may hold values from 0 to 255
- leaf: int32 [32768], P(('rows', 'feat')), may hold values from 0 to 1
- grad: bfloat16 [32, 32768], P(None, ('rows', 'feat')), may hold values from -15.55 to 15.55
- hess: bfloat16 [32, 32768], P(None, ('rows', 'feat')), may hold values from 0.049804688 to 1
Outputs:
- gains: float32 [256, 2, 256], P(('rows', 'feat'))
- best: float32 [2], replicated
The draws below stay inside these ranges and needn't reach their ends.
All inputs are finite; a program needn't handle non-finite values.
Results may differ from the reference program's by a relative error of at most 0.0003.
Values may be sent and summed in bfloat16 or wider, within the bound.
A program may use at most 128 MiB of HBM per device.

```python
import math
import jax
import jax.numpy as jnp
from jax import lax

F = 256
B = 256
K = 32
LEAVES = 2
ROWS = 32768


def draw_grad(key, part):
    offset_key = jax.random.fold_in(key, 11)
    noise_key = jax.random.fold_in(key, 23)
    offset = jax.random.uniform(offset_key, (K, 1), jnp.float32, -0.25, 0.25)
    position = jnp.arange(ROWS, dtype=jnp.float32)[None, :] / max(ROWS - 1, 1)
    spread = 1.0 + 2.0 * position
    noise = jax.random.truncated_normal(noise_key, -4.0, 4.0, (K, ROWS), jnp.float32)
    return (offset + spread * noise).astype(jnp.bfloat16)


def plant(values, key, low, high):
    extent = values.shape
    spot = [jax.random.randint(jax.random.fold_in(key, axis), (), 0, extent[axis]) for axis in range(len(extent))]
    values = values.at[tuple(spot)].set(low)
    longest = extent.index(max(extent))
    spot[longest] = (spot[longest] + 1) % extent[longest]
    return values.at[tuple(spot)].set(high)


def levels(rng, shape, pieces, low, largest):
    factor_of = 1.0
    for dim, blocks in pieces:
        heights = jax.random.uniform(jax.random.fold_in(jax.random.fold_in(rng, 6), dim), (blocks,), jnp.float32, low / len(pieces), largest / len(pieces))
        factor_of = factor_of * jnp.repeat(jnp.exp(heights), shape[dim] // blocks).reshape((-1,) + (1,) * (len(shape) - 1 - dim))
    return factor_of


def setup_inputs(seed: int = 0) -> dict:
    key_of = jax.random.split(jax.random.key(seed), 5)
    bins = plant(jax.random.randint(key_of[0], (F, ROWS), 0, B), jax.random.fold_in(key_of[0], 1), 0, B - 1).astype(jnp.int32)
    leaf = plant(jax.random.randint(key_of[1], (ROWS,), 0, LEAVES), jax.random.fold_in(key_of[1], 1), 0, LEAVES - 1).astype(jnp.int32)
    grad = draw_grad(jax.random.fold_in(key_of[4], 71), 0)
    hess = jnp.clip(jnp.exp(math.log(1.0) - 2.9996462 * jax.random.uniform(key_of[3], (K, ROWS), jnp.float32) ** levels(key_of[3], (K, ROWS), ((1, 32),), -0.2, 0.2)), 0.049804688, 1.0).astype(jnp.bfloat16)
    return dict(bins=bins, leaf=leaf, grad=grad, hess=hess)


def split_gains(hist, totals):
    count = hist.shape[0]
    cum = jnp.cumsum(hist, axis=1).reshape(count, B, LEAVES, 2, K)
    tot = totals.reshape(LEAVES, 2, K)
    left_grad = cum[:, :, :, 0, :]
    left_hess = cum[:, :, :, 1, :]
    all_grad = tot[:, 0, :]
    all_hess = tot[:, 1, :]
    right_grad = all_grad - left_grad
    right_hess = all_hess - left_hess
    score = left_grad * left_grad / (left_hess + 1.0) + right_grad * right_grad / (right_hess + 1.0) - all_grad * all_grad / (all_hess + 1.0)
    gains = (0.5 / K) * jnp.sum(score, axis=-1)
    return jnp.transpose(gains, (0, 2, 1))


def reference(bins, leaf, grad, hess):
    both = jnp.concatenate([grad, hess], axis=0).astype(jnp.float32)
    nodes = jnp.arange(LEAVES, dtype=jnp.int32)
    hot = (leaf[None, :] == nodes[:, None]).astype(jnp.float32)
    weighted = (hot[:, None, :] * both[None, :, :]).reshape(LEAVES * 2 * K, ROWS).T

    def one_feature(codes):
        return jax.ops.segment_sum(weighted, codes, num_segments=B)

    hist = lax.map(one_feature, bins)
    totals = jnp.sum(weighted, axis=0)
    gains = split_gains(hist, totals)
    best = jnp.max(gains, axis=(0, 2))
    return gains, best
```

```python
import functools

import jax
import jax.numpy as jnp
from jax import lax
from jax.experimental import pallas as pl
from jax.experimental.pallas import tpu as pltpu
from jax.sharding import PartitionSpec as P

B = 256
LEAVES = 2
LANES = 128
WIDE = 256
GROUP = 16
OFFSET = 32768
AHEAD = 6
MESH = pl.DeviceIdType.MESH


def accumulator(mxu, height):
    return pltpu.ACC(mxu)((height, B), jnp.float32)


def feature_gains(cum, outputs):
    rows = []
    for leaf in range(LEAVES):
        base = leaf * 2 * outputs
        left_grad = cum[base:base + outputs]
        left_hess = cum[base + outputs:base + 2 * outputs]
        all_grad = left_grad[:, B - 1:B]
        all_hess = left_hess[:, B - 1:B]
        right_grad = all_grad - left_grad
        right_hess = all_hess - left_hess
        score = (
            left_grad * left_grad / (left_hess + 1.0)
            + right_grad * right_grad / (right_hess + 1.0)
            - all_grad * all_grad / (all_hess + 1.0)
        )
        rows.append(0.5 / outputs * jnp.sum(score, axis=0, keepdims=True))
    return jnp.concatenate(rows, axis=0)


def kernel(sizes, outputs, shard, owned, *refs):
    half = owned // 2
    height = LEAVES * 2 * outputs
    pl.run_scoped(
        functools.partial(body, sizes, outputs, shard, owned, refs),
        *[accumulator(0, height)] * half,
        *[accumulator(1, height)] * half,
        pltpu.VMEM((shard // LANES, height, LANES), jnp.bfloat16),
        pltpu.VMEM((half, shard, LANES), jnp.int16),
        pltpu.VMEM((shard, owned), jnp.int16),
    )


def body(sizes, outputs, shard, owned, refs, *scoped):
    (bins_ref, leaf_ref, grad_ref, hess_ref, gains_ref, best_ref,
     codes_in, codes_all, packed_all, best_all, send_c, recv_c, send_g, recv_g, send_b, recv_b) = refs
    accs = scoped[:owned]
    lhs_ref, tile_ref, cols_ref = scoped[owned:]
    na, nb, nz = sizes
    pairs = na * nb * nz
    count = 2 * pairs
    r = lax.axis_index("rows")
    f = lax.axis_index("feat")
    a, b = r // nb, r % nb
    z, c = f // 2, f % 2

    group = na * nb

    def place(pa, pb, pz, pc):
        return {"rows": pa * nb + pb, "feat": pz * 2 + pc}

    def line(pa, pb, pz, pc):
        return ((pa * nb + pb) * nz + pz) * 2 + pc

    def toggled(dz):
        value, bit = 0, 1
        while bit < nz:
            value = value + (z // bit + dz // bit) % 2 * bit
            bit *= 2
        return value

    def offsets(p, pc):
        da = (1 - pc) * ((p // nb) % na) + pc * (p % na)
        db = (1 - pc) * (p % nb) + pc * ((p // na) % nb)
        return da, db, p // group

    me = line(a, b, z, c)
    other = 1 - c

    def source(p, pc):
        da, db, dz = offsets(p, pc)
        return line((a + da) % na, (b + db) % nb, toggled(dz), pc)

    def target(s):
        da, db, dz = offsets(s // 2, c)
        return (a + na - da) % na, (b + nb - db) % nb, toggled(dz), (c + s) % 2

    rows_size, feat_size = na * nb, nz * 2
    row_at = [lax.rem(r + i, rows_size) for i in range(rows_size)]
    feat_at = [lax.rem(f + i, feat_size) for i in range(feat_size)]
    others = [(i, j) for i in range(rows_size) for j in range(feat_size) if i + j > 0]

    barrier = pltpu.get_barrier_semaphore()
    for i, j in others:
        pl.semaphore_signal(
            barrier, inc=1, device_id={"rows": row_at[i], "feat": feat_at[j]}, device_id_type=MESH)

    chunks = shard // LANES
    own = packed_all.at[me]
    for j in range(chunks):
        part = slice(j * LANES, (j + 1) * LANES)
        own[2 * j * outputs:(2 * j + 1) * outputs] = grad_ref[:, part]
        own[(2 * j + 1) * outputs:(2 * j + 2) * outputs] = hess_ref[:, part]
    node = leaf_ref[...].astype(jnp.float32)
    node = jnp.concatenate([node, jnp.zeros((-chunks % 16, LANES), jnp.float32)], axis=0)
    own[2 * chunks * outputs:] = node.astype(jnp.bfloat16)
    codes_in[...] = bins_ref[...].astype(jnp.int16).reshape(codes_in.shape)

    half = owned // 2
    width = 2 * outputs
    tiles = [(t, p) for t in range(shard // WIDE) for p in range(half)]
    lane_id = lax.broadcasted_iota(jnp.int32, (GROUP, LANES), 1)
    low_top = [(lane_id + h).astype(jnp.int16) for h in range(0, B, LANES)]
    high_top = [((lane_id + h) * B + (B - 1 - OFFSET)).astype(jnp.int16) for h in range(0, B, LANES)]
    one = jnp.ones((GROUP, LANES), jnp.bfloat16)
    none = jnp.zeros((GROUP, LANES), jnp.bfloat16)

    def columns(blocks):
        parts = []
        for codes in blocks:
            wide = codes.astype(jnp.int32)
            parts.append(wide[:half] + wide[half:] * B - OFFSET)
        cols_ref[:, :half * len(blocks)] = jnp.concatenate(parts, axis=0).T.astype(jnp.int16)

    def spread(t, p, at):
        for row in range(t * WIDE, (t + 1) * WIDE, GROUP):
            tile_ref[p, row:row + GROUP] = jnp.broadcast_to(
                cols_ref[row:row + GROUP, at + p:at + p + 1], (GROUP, LANES))

    def weigh(where, t):
        for j in range(t * WIDE // LANES, (t + 1) * WIDE // LANES):
            both = packed_all[where, j * width:(j + 1) * width]
            node = packed_all[where, chunks * width + j:chunks * width + j + 1]
            zero = jnp.zeros_like(both)
            for leaf in range(LEAVES):
                lhs_ref[j, leaf * width:(leaf + 1) * width] = jnp.where(node == leaf, both, zero)

    def push(k):
        t, p = tiles[k % len(tiles)]
        low, high = [], []
        for row in range(t * WIDE, (t + 1) * WIDE, GROUP):
            code = tile_ref[p, row:row + GROUP]
            rest = code & (B - 1)
            low.append(jnp.concatenate([jnp.where(rest <= top, one, none) for top in low_top], axis=1))
            high.append(jnp.concatenate([jnp.where(code <= top, one, none) for top in high_top], axis=1))
        pltpu.matmul_push_rhs(jnp.concatenate(low, axis=0), k % 2, 0)
        pltpu.matmul_push_rhs(jnp.concatenate(high, axis=0), k % 2, 1)

    def add_block(later, at):
        for k, (t, p) in enumerate(tiles):
            if k + 1 < len(tiles):
                push(k + 1)
            span = range(t * WIDE // LANES, (t + 1) * WIDE // LANES)
            lhs = jnp.concatenate([lhs_ref[j] for j in span], axis=1)
            pltpu.matmul_acc_lhs(accs[p], lhs, load_staged_rhs=k % 2)
            pltpu.matmul_acc_lhs(accs[half + p], lhs, load_staged_rhs=k % 2)
            spread(t, p, at)
            if p == half - 1:
                weigh(later, t)
        push(len(tiles))

    for acc in accs:
        pltpu.matmul_pop(acc)

    pl.semaphore_wait(barrier, count - 1)

    def packed_copy(src, slot, sem, where):
        return pltpu.make_async_remote_copy(
            src_ref=src, dst_ref=packed_all.at[slot], send_sem=send_g.at[sem], recv_sem=recv_g.at[slot],
            device_id=where, device_id_type=MESH)

    def codes_copy(s):
        where = target(s)
        return pltpu.make_async_remote_copy(
            src_ref=codes_in.at[line(*where)], dst_ref=codes_all.at[me], send_sem=send_c.at[s],
            recv_sem=recv_c.at[me], device_id=place(*where), device_id_type=MESH)

    def best_copy(i, j):
        return pltpu.make_async_remote_copy(
            src_ref=best_all.at[me], dst_ref=best_all.at[me], send_sem=send_b.at[i * feat_size + j],
            recv_sem=recv_b.at[me], device_id={"rows": row_at[i], "feat": feat_at[j]}, device_id_type=MESH)

    def forward(p, block, slot):
        for core in range(2):
            n1, n2 = (nb, na) if core == 0 else (na, nb)

            def spot(step, k):
                along_b = (step == 1) == (core == 0)
                if along_b:
                    return place(a, (b + nb - k) % nb, z, c)
                return place((a + na - k) % na, b, z, c)

            @pl.when(jnp.logical_and(c == core, (p // n1) % n2 == 0))
            def _():
                for k in range(1, n2):
                    sem = nz * n1 + (p // group * n1 + p % n1) * (n2 - 1) + k - 1
                    packed_copy(block, slot, sem, spot(2, k)).start()

            @pl.when(jnp.logical_and(c == core, p % group == 0))
            def _():
                for k in range(1, n1):
                    packed_copy(block, slot, nz + p // group * (n1 - 1) + k - 1, spot(1, k)).start()

        packed_copy(block, slot, nz * group + p, place(a, b, z, other)).start()

    def take(p):
        slot = source(p, c)
        packed_copy(own, slot, 0, place(a, b, z, other)).wait_recv()
        forward(p, packed_all.at[slot], slot)

    for k in range(1, nz):
        packed_copy(own, me, k, place(a, b, toggled(k), c)).start()
    forward(jnp.int32(0), own, me)

    for s in range(1, min(2 * AHEAD, count)):
        codes_copy(s).start()

    columns([codes_in[me]])
    for t, p in tiles:
        spread(t, p, 0)
        if p == half - 1:
            weigh(me, t)
    push(0)

    def wait_codes(here):
        pltpu.make_async_remote_copy(
            src_ref=codes_all.at[here], dst_ref=codes_all.at[here], send_sem=send_c.at[0],
            recv_sem=recv_c.at[here], device_id=place(a, b, z, other), device_id_type=MESH).wait_recv()

    @pl.loop(0, pairs)
    def _(i):
        @pl.when(i + AHEAD < pairs)
        def _():
            for k in range(2):
                codes_copy(2 * (i + AHEAD) + k).start()

        @pl.when(jnp.logical_and((i + 1) % group > 0, i + 1 < pairs))
        def _():
            take(i + 1)

        @pl.when(jnp.logical_and(i % group == group - 2, i + 2 < pairs))
        def _():
            take(i + 2)

        beside = source(i, other)
        wait_codes(beside)
        packed_copy(own, beside, 0, place(a, b, z, other)).wait_recv()
        later = source(jnp.minimum(i + 1, pairs - 1), c)

        @pl.when(i + 1 < pairs)
        def _():
            wait_codes(later)

        columns([codes_all[beside], codes_all[later]])
        add_block(beside, 0)
        add_block(later, half)

    for acc in (accs[0], accs[half]):
        pltpu.matmul_acc_lhs(acc, jnp.zeros((LEAVES * width, WIDE), jnp.bfloat16), load_staged_rhs=0)

    top = None
    for i in range(owned):
        value = feature_gains(pltpu.matmul_pop(accs[i]), outputs)
        gains_ref[i] = value
        top = value if top is None else jnp.maximum(top, value)
    peak = jnp.max(top, axis=1, keepdims=True)
    lane = lax.broadcasted_iota(jnp.int32, (1, LANES), 1)
    best_all[me] = jnp.where(lane < LANES // 2, peak[0:1], peak[1:2])

    @pl.loop(1, count)
    def _(s):
        pltpu.make_async_remote_copy(
            src_ref=codes_in.at[0], dst_ref=codes_all.at[0], send_sem=send_c.at[s],
            recv_sem=recv_c.at[0], device_id=place(a, b, z, other), device_id_type=MESH).wait_send()
        packed_copy(own, me, s, place(a, b, z, other)).wait_send()

    for i, j in others:
        best_copy(i, j).start()

    @pl.loop(0, count)
    def _(here):
        @pl.when(here != me)
        def _():
            pltpu.make_async_remote_copy(
                src_ref=best_all.at[here], dst_ref=best_all.at[here], send_sem=send_b.at[0],
                recv_sem=recv_b.at[here], device_id=place(a, b, z, other), device_id_type=MESH).wait_recv()

    for i, j in others:
        best_copy(i, j).wait_send()

    best_ref[...] = jnp.max(best_all[...], axis=0)


def shards(sizes, bins, leaf, grad, hess):
    na, nb, nz = sizes
    count = na * nb * nz * 2
    outputs = grad.shape[0]
    features, shard = bins.shape
    owned = features // count
    chunks = shard // LANES
    packed_rows = chunks * 2 * outputs + chunks + -chunks % 16
    codes_shape = (count, owned, shard)
    dma = pltpu.SemaphoreType.DMA((count,))
    gains, best = pl.pallas_call(
        functools.partial(kernel, sizes, outputs, shard, owned),
        out_shape=(
            jax.ShapeDtypeStruct((owned, LEAVES, B), jnp.float32),
            jax.ShapeDtypeStruct((1, LANES), jnp.float32),
        ),
        in_specs=[pl.BlockSpec(memory_space=pltpu.VMEM)] * 4,
        out_specs=(pl.BlockSpec(memory_space=pltpu.VMEM),) * 2,
        scratch_shapes=[
            pltpu.VMEM(codes_shape, jnp.int16),
            pltpu.VMEM(codes_shape, jnp.int16),
            pltpu.VMEM((count, packed_rows, LANES), jnp.bfloat16),
            pltpu.VMEM((count, 1, LANES), jnp.float32),
            dma, dma, dma, dma, dma, dma,
        ],
        compiler_params=pltpu.CompilerParams(
            collective_id=0, has_side_effects=True, vmem_limit_bytes=56 * 1024 * 1024
        ),
    )(bins, leaf.reshape(chunks, LANES), grad, hess)
    return gains, best[0, ::LANES // LEAVES]


def solution(mesh):
    rows, feat = mesh.shape["rows"], mesh.shape["feat"]
    sizes = (rows // 2, 2, feat // 2)
    return jax.shard_map(
        functools.partial(shards, sizes),
        mesh=mesh,
        in_specs=(
            P(None, ("rows", "feat")),
            P(("rows", "feat")),
            P(None, ("rows", "feat")),
            P(None, ("rows", "feat")),
        ),
        out_specs=(P(("rows", "feat"), None, None), P()),
        check_vma=False,
    )
```

```python
import functools

import jax
import jax.numpy as jnp
from jax import lax
from jax.experimental import pallas as pl
from jax.experimental.pallas import tpu as pltpu
from jax.sharding import PartitionSpec as P

B = 256
LEAVES = 2
LANES = 128
WIDE = 256
GROUP = 16
OFFSET = 32768
AHEAD = 5
PARTS = 2
MESH = pl.DeviceIdType.MESH


def accumulator(mxu, height):
    return pltpu.ACC(mxu)((height, B), jnp.float32)


def feature_gains(cum, outputs):
    rows = []
    for leaf in range(LEAVES):
        base = leaf * 2 * outputs
        left_grad = cum[base:base + outputs]
        left_hess = cum[base + outputs:base + 2 * outputs]
        all_grad = left_grad[:, B - 1:B]
        all_hess = left_hess[:, B - 1:B]
        right_grad = all_grad - left_grad
        right_hess = all_hess - left_hess
        score = (
            left_grad * left_grad / (left_hess + 1.0)
            + right_grad * right_grad / (right_hess + 1.0)
            - all_grad * all_grad / (all_hess + 1.0)
        )
        rows.append(0.5 / outputs * jnp.sum(score, axis=0, keepdims=True))
    return jnp.concatenate(rows, axis=0)


def kernel(sizes, outputs, shard, owned, *refs):
    na, nb, nz = sizes
    half = owned // 2
    height = LEAVES * 2 * outputs
    count = na * nb * nz * 2
    sends = PARTS * (2 * nz + 2 * nz * max(na, nb) * (na + nb))
    dma = pltpu.SemaphoreType.DMA((count,))
    one = pltpu.SemaphoreType.DMA
    pl.run_scoped(
        functools.partial(body, sizes, outputs, shard, owned, refs),
        *[accumulator(0, height)] * half,
        *[accumulator(1, height)] * half,
        pltpu.VMEM((shard // LANES, height, LANES), jnp.bfloat16),
        pltpu.VMEM((half, shard, LANES), jnp.int16),
        pltpu.VMEM((shard, owned), jnp.int16),
        pltpu.SemaphoreType.DMA((2 * shard // LANES + 2,)),
        dma, dma,
        pltpu.SemaphoreType.DMA((sends,)),
        pltpu.SemaphoreType.DMA((count, PARTS)),
        dma, one, one,
    )


def body(sizes, outputs, shard, owned, refs, *scoped):
    (bins_ref, leaf_ref, grad_ref, hess_ref, gains_ref, best_ref,
     bins_in, leaf_in, codes_in, codes_all, packed_all, best_all) = refs
    accs = scoped[:owned]
    (lhs_ref, tile_ref, cols_ref,
     load, send_c, recv_c, send_g, recv_g, send_s, send_b, recv_b) = scoped[owned:]
    na, nb, nz = sizes
    group = na * nb
    pairs = group * nz
    count = 2 * pairs
    chunks = shard // LANES
    half = owned // 2
    width = 2 * outputs
    nodes = chunks + -chunks % 16
    r = lax.axis_index("rows")
    f = lax.axis_index("feat")
    a, b = r // nb, r % nb
    z, c = f // 2, f % 2
    other = 1 - c

    def place(pa, pb, pz, pc):
        return {"rows": pa * nb + pb, "feat": pz * 2 + pc}

    def line(pa, pb, pz, pc):
        return ((pa * nb + pb) * nz + pz) * 2 + pc

    def toggled(dz):
        value, bit = 0, 1
        while bit < nz:
            value = value + lax.rem(lax.div(z, bit) + lax.div(dz, bit), 2) * bit
            bit *= 2
        return value

    def offsets(p, pc):
        p = jnp.int32(p)
        da = (1 - pc) * lax.rem(lax.div(p, nb), na) + pc * lax.rem(p, na)
        db = (1 - pc) * lax.rem(p, nb) + pc * lax.rem(lax.div(p, na), nb)
        return da, db, lax.div(p, group)

    me = line(a, b, z, c)
    beside_me = place(a, b, z, other)

    def source(p, pc):
        da, db, dz = offsets(p, pc)
        return line(lax.rem(a + da, na), lax.rem(b + db, nb), toggled(dz), pc)

    barrier = pltpu.get_barrier_semaphore()

    def greet(where):
        pl.semaphore_signal(barrier, inc=1, device_id=where, device_id_type=MESH)

    for step in (1, -1):
        @pl.when(jnp.logical_and(z + step >= 0, z + step < nz))
        def _():
            for pc in range(2):
                greet(place(a, b, z + step, pc))
    for i in range(na):
        for j in range(nb):
            for k in range(2):
                if i + j + k > 0:
                    greet(place((a + i) % na, (b + j) % nb, z, (c + k) % 2))

    def spots(j):
        start = j * width + (j >= chunks // PARTS) * nodes
        return start, start + outputs, start + width

    node_rows = chunks // PARTS * width
    cuts = [0, node_rows + nodes, chunks * width + nodes]
    loads = [pltpu.make_async_copy(leaf_ref, leaf_in, load.at[2 * chunks])]
    for j in range(chunks):
        part = slice(j * LANES, (j + 1) * LANES)
        start, middle, end = spots(j)
        loads.append(pltpu.make_async_copy(
            grad_ref.at[:, part], packed_all.at[me, start:middle], load.at[2 * j]))
        loads.append(pltpu.make_async_copy(
            hess_ref.at[:, part], packed_all.at[me, middle:end], load.at[2 * j + 1]))
    load_bins = pltpu.make_async_copy(bins_ref, bins_in, load.at[2 * chunks + 1])
    for copy in loads:
        copy.start()
    load_bins.start()

    lane_id = lax.broadcasted_iota(jnp.int32, (GROUP, LANES), 1)
    low_top = [(lane_id + h).astype(jnp.int16) for h in range(0, B, LANES)]
    high_top = [((lane_id + h) * B + (B - 1 - OFFSET)).astype(jnp.int16) for h in range(0, B, LANES)]
    one = jnp.ones((GROUP, LANES), jnp.bfloat16)
    none = jnp.zeros((GROUP, LANES), jnp.bfloat16)
    tiles = [(t, p) for t in range(shard // WIDE) for p in range(half)]

    def columns(blocks):
        parts = []
        for codes in blocks:
            wide = codes.astype(jnp.int32)
            parts.append(wide[:half] + wide[half:] * B - OFFSET)
        cols_ref[:, :half * len(blocks)] = jnp.concatenate(parts, axis=0).T.astype(jnp.int16)

    def spread(t, p, at):
        for row in range(t * WIDE, (t + 1) * WIDE, GROUP):
            tile_ref[p, row:row + GROUP] = jnp.broadcast_to(
                cols_ref[row:row + GROUP, at + p:at + p + 1], (GROUP, LANES))

    def weigh(where, t):
        for j in range(t * WIDE // LANES, (t + 1) * WIDE // LANES):
            start, _, end = spots(j)
            both = packed_all[where, start:end]
            node = packed_all[where, node_rows + j:node_rows + j + 1]
            zero = jnp.zeros_like(both)
            for leaf in range(LEAVES):
                lhs_ref[j, leaf * width:(leaf + 1) * width] = jnp.where(node == leaf, both, zero)

    def push(k):
        t, p = tiles[k % len(tiles)]
        low, high = [], []
        for row in range(t * WIDE, (t + 1) * WIDE, GROUP):
            code = tile_ref[p, row:row + GROUP]
            rest = code & (B - 1)
            low.append(jnp.concatenate([jnp.where(rest <= top, one, none) for top in low_top], axis=1))
            high.append(jnp.concatenate([jnp.where(code <= top, one, none) for top in high_top], axis=1))
        pltpu.matmul_push_rhs(jnp.concatenate(low, axis=0), k % 2, 0)
        pltpu.matmul_push_rhs(jnp.concatenate(high, axis=0), k % 2, 1)

    def add_block(later, at):
        for k, (t, p) in enumerate(tiles):
            if k + 1 < len(tiles):
                push(k + 1)
            span = range(t * WIDE // LANES, (t + 1) * WIDE // LANES)
            lhs = jnp.concatenate([lhs_ref[j] for j in span], axis=1)
            pltpu.matmul_acc_lhs(accs[p], lhs, load_staged_rhs=k % 2)
            pltpu.matmul_acc_lhs(accs[half + p], lhs, load_staged_rhs=k % 2)
            if later is not None:
                spread(t, p, at)
                if p == half - 1:
                    weigh(later, t)
        if later is not None:
            push(len(tiles))

    for acc in accs:
        pltpu.matmul_pop(acc)

    sent = []

    def packed_copy(slot, sem, where, part):
        rows = slice(cuts[part], cuts[part + 1])
        return pltpu.make_async_remote_copy(
            src_ref=packed_all.at[slot, rows], dst_ref=packed_all.at[slot, rows], send_sem=send_g.at[sem],
            recv_sem=recv_g.at[slot, part], device_id=where, device_id_type=MESH)

    def wait_packed(slot, part):
        packed_copy(slot, 0, beside_me, part).wait_recv()

    def send_packed(slot, where, part, when):
        sem = len(sent)
        sent.append((part, when))
        copy = packed_copy(slot, sem, where, part)
        pl.when(when())(copy.start)

    def beside_copy(slot, p):
        return pltpu.make_async_remote_copy(
            src_ref=packed_all.at[slot], dst_ref=packed_all.at[slot], send_sem=send_s.at[p],
            recv_sem=recv_g.at[slot, 0], device_id=beside_me, device_id_type=MESH)

    def send_codes(q, mine=True):
        da, db, dz = offsets(q, c)
        ta, tb, tz = lax.rem(a + na - da, na), lax.rem(b + nb - db, nb), toggled(dz)
        base = line(ta, tb, tz, 0)
        for k in range(0 if mine else 1, 2):
            pc = other if k else c
            pltpu.make_async_remote_copy(
                src_ref=codes_in.at[base + pc], dst_ref=codes_all.at[me], send_sem=send_c.at[2 * q + k],
                recv_sem=recv_c.at[me], device_id=place(ta, tb, tz, pc), device_id_type=MESH).start()

    def is_core(core):
        return c == core

    def passes(step, k):
        origin, there = z - step * k, z + step
        return jnp.logical_and(
            jnp.logical_and(origin >= 0, origin < nz), jnp.logical_and(there >= 0, there < nz))

    def in_plane(g, q, part):
        slot = source(g * group + q, c)
        for core in range(2):
            n1, n2 = (nb, na) if core == 0 else (na, nb)

            def spot(step, k):
                if (step == 1) == (core == 0):
                    return place(a, (b + nb - k) % nb, z, c)
                return place((a + na - k) % na, b, z, c)

            if q < n1:
                for k in range(1, n2):
                    send_packed(slot, spot(2, k), part, functools.partial(is_core, core))
            if q == 0:
                for k in range(1, n1):
                    send_packed(slot, spot(1, k), part, functools.partial(is_core, core))

    def along(k, part):
        for step in (1, -1):
            origin, there = z - step * k, z + step
            inside = jnp.logical_and(origin >= 0, origin < nz)
            slot = line(a, b, origin, c)
            if k > 0:
                @pl.when(inside)
                def _():
                    wait_packed(slot, part)
            send_packed(slot, place(a, b, there, c), part, functools.partial(passes, step, k))

    def relay(g, ahead):
        for part in range(PARTS):
            for q in range(1, early):
                wait_packed(source(g * group + q, c), part)
                in_plane(g, q, part)
            if ahead < nz:
                along(ahead, part)
                in_plane(ahead, 0, part)
        for q in range(1, early):
            beside_copy(source(g * group + q, c), g * group + q).start()
        if ahead < nz:
            beside_copy(source(ahead * group, c), ahead * group).start()

    early = max(na, nb)
    around = 2 * group - 1 + 2 * jnp.where(z > 0, 1, 0) + 2 * jnp.where(z + 1 < nz, 1, 0)

    loads[0].wait()
    node = jnp.concatenate(
        [leaf_in[...].astype(jnp.float32), jnp.zeros((nodes - chunks, LANES), jnp.float32)], axis=0)
    packed_all[me, node_rows:node_rows + nodes] = node.astype(jnp.bfloat16)
    for copy in loads[1:]:
        copy.wait()

    pl.semaphore_wait(barrier, around)

    for part in range(PARTS):
        along(0, part)
        in_plane(0, 0, part)
    beside_copy(me, 0).start()

    load_bins.wait()
    codes_in[...] = bins_in[...].astype(jnp.int16).reshape(codes_in.shape)
    for q in range(min(AHEAD, group)):
        send_codes(q, q > 0)

    def wait_codes(here):
        pltpu.make_async_remote_copy(
            src_ref=codes_all.at[here], dst_ref=codes_all.at[here], send_sem=send_c.at[0],
            recv_sem=recv_c.at[here], device_id=beside_me, device_id_type=MESH).wait_recv()

    def wait_beside(beside):
        wait_codes(beside)
        pltpu.make_async_remote_copy(
            src_ref=packed_all.at[beside], dst_ref=packed_all.at[beside], send_sem=send_s.at[0],
            recv_sem=recv_g.at[beside, 0], device_id=beside_me, device_id_type=MESH).wait_recv()

    columns([codes_in[me]])
    for t, p in tiles:
        spread(t, p, 0)
        if p == half - 1:
            weigh(me, t)
    push(0)

    beside = source(0, other)
    wait_beside(beside)
    columns([codes_all[beside]])
    add_block(beside, 0)
    relay(0, 1)
    for q in range(min(AHEAD, group), min(AHEAD, pairs)):
        send_codes(q)
    later = source(1, c)
    wait_codes(later)
    columns([codes_all[later]])
    add_block(later, 0)

    def step(i, slots):
        beside, later = slots
        for g in range(nz - 1):
            @pl.when(i == g * group + group - 2)
            def _():
                relay(g + 1, g + 2)

        @pl.when(lax.rem(i + 1, group) >= early)
        def _():
            for part in range(PARTS):
                wait_packed(later, part)
            beside_copy(later, i + 1).start()

        @pl.when(i + AHEAD <= pairs)
        def _():
            send_codes(i + AHEAD - 1)

        wait_beside(beside)
        wait_codes(later)
        columns([codes_all[beside], codes_all[later]])
        add_block(beside, 0)
        add_block(later, half)
        return source(i + 1, other), source(i + 2, c)

    beside, _ = lax.fori_loop(1, pairs - 1, step, (source(1, other), source(2, c)))
    wait_beside(beside)
    columns([codes_all[beside]])
    add_block(beside, 0)
    add_block(None, 0)

    top = None
    for i in range(owned):
        value = feature_gains(pltpu.matmul_pop(accs[i]), outputs)
        for h in range(B // LANES):
            row = (i * (B // LANES) + h) * LEAVES
            gains_ref[row:row + LEAVES] = value[:, h * LANES:(h + 1) * LANES]
        top = value if top is None else jnp.maximum(top, value)
    peak = jnp.max(top, axis=1, keepdims=True)
    lane = lax.broadcasted_iota(jnp.int32, (1, LANES), 1)
    best_all[me] = jnp.where(lane == 0, peak[0:1], peak[1:2])

    others = [(i, j) for i in range(group) for j in range(nz * 2) if i + j > 0]
    for i, j in reversed(others):
        pltpu.make_async_remote_copy(
            src_ref=best_all.at[me], dst_ref=best_all.at[me], send_sem=send_b, recv_sem=recv_b,
            device_id={"rows": lax.rem(r + i, group), "feat": lax.rem(f + j, nz * 2)},
            device_id_type=MESH).start()

    @pl.loop(1, count)
    def _(s):
        pltpu.make_async_remote_copy(
            src_ref=codes_in.at[0], dst_ref=codes_all.at[0], send_sem=send_c.at[s],
            recv_sem=recv_c.at[0], device_id=beside_me, device_id_type=MESH).wait_send()

    @pl.loop(0, pairs)
    def _(p):
        beside_copy(me, p).wait_send()

    for sem, (part, when) in enumerate(sent):
        pl.when(when())(packed_copy(me, sem, beside_me, part).wait_send)

    rest = best_all.at[0:count - 1]
    bests = pltpu.make_async_remote_copy(
        src_ref=rest, dst_ref=rest, send_sem=send_b, recv_sem=recv_b,
        device_id=beside_me, device_id_type=MESH)
    bests.wait_recv()
    bests.wait_send()

    best_ref[...] = jnp.max(best_all[...], axis=0)[:, :LEAVES]


def shards(sizes, bins, leaf, grad, hess):
    na, nb, nz = sizes
    count = na * nb * nz * 2
    outputs = grad.shape[0]
    features, shard = bins.shape
    owned = features // count
    chunks = shard // LANES
    packed_rows = chunks * 2 * outputs + chunks + -chunks % 16
    codes_shape = (count, owned, shard)
    halves = B // LANES
    gains, best = pl.pallas_call(
        functools.partial(kernel, sizes, outputs, shard, owned),
        out_shape=(
            jax.ShapeDtypeStruct((owned * halves * LEAVES, LANES), jnp.float32),
            jax.ShapeDtypeStruct((1, LEAVES), jnp.float32),
        ),
        in_specs=[pl.BlockSpec(memory_space=pl.ANY)] * 4,
        out_specs=(pl.BlockSpec(memory_space=pltpu.VMEM),) * 2,
        scratch_shapes=[
            pltpu.VMEM((features, shard), jnp.int32),
            pltpu.VMEM((chunks, LANES), jnp.int32),
            pltpu.VMEM(codes_shape, jnp.int16),
            pltpu.VMEM(codes_shape, jnp.int16),
            pltpu.VMEM((count, packed_rows, LANES), jnp.bfloat16),
            pltpu.VMEM((count, 1, LANES), jnp.float32),
        ],
        compiler_params=pltpu.CompilerParams(
            collective_id=0, has_side_effects=True, vmem_limit_bytes=56 * 1024 * 1024
        ),
    )(bins, leaf.reshape(chunks, LANES), grad, hess)
    gains = gains.reshape(owned, halves, LEAVES, LANES).transpose(0, 2, 1, 3).reshape(owned, LEAVES, B)
    return gains, best.reshape(LEAVES)


def solution(mesh):
    rows, feat = mesh.shape["rows"], mesh.shape["feat"]
    sizes = (rows // 2, 2, feat // 2)
    return jax.shard_map(
        functools.partial(shards, sizes),
        mesh=mesh,
        in_specs=(
            P(None, ("rows", "feat")),
            P(("rows", "feat")),
            P(None, ("rows", "feat")),
            P(None, ("rows", "feat")),
        ),
        out_specs=(P(("rows", "feat"), None, None), P()),
        check_vma=False,
    )
```

```python
import functools

import jax
import jax.numpy as jnp
from jax import lax
from jax.experimental import pallas as pl
from jax.experimental.pallas import tpu as pltpu
from jax.sharding import PartitionSpec as P

B = 256
LEAVES = 2
LANES = 128
WIDE = 256
GROUP = 16
OFFSET = 32768
PARTS = 2
MESH = pl.DeviceIdType.MESH


def accumulator(mxu, height):
    return pltpu.ACC(mxu)((height, B), jnp.float32)


def feature_gains(cum, outputs):
    rows = []
    for leaf in range(LEAVES):
        base = leaf * 2 * outputs
        left_grad = cum[base:base + outputs]
        left_hess = cum[base + outputs:base + 2 * outputs]
        all_grad = left_grad[:, B - 1:B]
        all_hess = left_hess[:, B - 1:B]
        right_grad = all_grad - left_grad
        right_hess = all_hess - left_hess
        score = (
            left_grad * left_grad / (left_hess + 1.0)
            + right_grad * right_grad / (right_hess + 1.0)
            - all_grad * all_grad / (all_hess + 1.0)
        )
        rows.append(0.5 / outputs * jnp.sum(score, axis=0, keepdims=True))
    return jnp.concatenate(rows, axis=0)


def kernel(sizes, outputs, shard, owned, *refs):
    na, nb, nz = sizes
    half = owned // 2
    height = LEAVES * 2 * outputs
    count = na * nb * nz * 2
    sends = PARTS * (2 * nz + 2 * nz * max(na, nb) * (na + nb))
    dma = pltpu.SemaphoreType.DMA((count,))
    one = pltpu.SemaphoreType.DMA
    pl.run_scoped(
        functools.partial(body, sizes, outputs, shard, owned, refs),
        *[accumulator(0, height)] * half,
        *[accumulator(1, height)] * half,
        pltpu.VMEM((shard // LANES, height, LANES), jnp.bfloat16),
        pltpu.VMEM((half, shard, LANES), jnp.int16),
        pltpu.VMEM((shard, owned), jnp.int16),
        pltpu.SemaphoreType.DMA((2 * shard // LANES + 2,)),
        dma, dma,
        pltpu.SemaphoreType.DMA((sends,)),
        pltpu.SemaphoreType.DMA((count, PARTS)),
        dma, one, one,
    )


def body(sizes, outputs, shard, owned, refs, *scoped):
    (bins_ref, leaf_ref, grad_ref, hess_ref, gains_ref, best_ref,
     bins_in, leaf_in, codes_in, codes_all, packed_all, best_all) = refs
    accs = scoped[:owned]
    (lhs_ref, tile_ref, cols_ref,
     load, send_c, recv_c, send_g, recv_g, send_s, send_b, recv_b) = scoped[owned:]
    na, nb, nz = sizes
    group = na * nb
    pairs = group * nz
    count = 2 * pairs
    chunks = shard // LANES
    half = owned // 2
    width = 2 * outputs
    nodes = chunks + -chunks % 16
    r = lax.axis_index("rows")
    f = lax.axis_index("feat")
    a, b = r // nb, r % nb
    z, c = f // 2, f % 2
    other = 1 - c

    def place(pa, pb, pz, pc):
        return {"rows": pa * nb + pb, "feat": pz * 2 + pc}

    def line(pa, pb, pz, pc):
        return ((pa * nb + pb) * nz + pz) * 2 + pc

    def toggled(dz):
        value, bit = 0, 1
        while bit < nz:
            value = value + lax.rem(lax.div(z, bit) + lax.div(dz, bit), 2) * bit
            bit *= 2
        return value

    def offsets(p, pc):
        p = jnp.int32(p)
        da = (1 - pc) * lax.rem(lax.div(p, nb), na) + pc * lax.rem(p, na)
        db = (1 - pc) * lax.rem(p, nb) + pc * lax.rem(lax.div(p, na), nb)
        return da, db, lax.div(p, group)

    me = line(a, b, z, c)
    beside_me = place(a, b, z, other)

    def source(p, pc):
        da, db, dz = offsets(p, pc)
        return line(lax.rem(a + da, na), lax.rem(b + db, nb), toggled(dz), pc)

    barrier = pltpu.get_barrier_semaphore()

    def greet(where):
        pl.semaphore_signal(barrier, inc=1, device_id=where, device_id_type=MESH)

    for step in (1, -1):
        @pl.when(jnp.logical_and(z + step >= 0, z + step < nz))
        def _():
            for pc in range(2):
                greet(place(a, b, z + step, pc))
    for i in range(na):
        for j in range(nb):
            for k in range(2):
                if i + j + k > 0:
                    greet(place((a + i) % na, (b + j) % nb, z, (c + k) % 2))

    def spots(j):
        start = j * width + (j >= chunks // PARTS) * nodes
        return start, start + outputs, start + width

    node_rows = chunks // PARTS * width
    cuts = [0, node_rows + nodes, chunks * width + nodes]
    loads = [pltpu.make_async_copy(leaf_ref, leaf_in, load.at[2 * chunks])]
    for j in range(chunks):
        part = slice(j * LANES, (j + 1) * LANES)
        start, middle, end = spots(j)
        loads.append(pltpu.make_async_copy(
            grad_ref.at[:, part], packed_all.at[me, start:middle], load.at[2 * j]))
        loads.append(pltpu.make_async_copy(
            hess_ref.at[:, part], packed_all.at[me, middle:end], load.at[2 * j + 1]))
    load_bins = pltpu.make_async_copy(bins_ref, bins_in, load.at[2 * chunks + 1])
    for copy in loads:
        copy.start()
    load_bins.start()

    lane_id = lax.broadcasted_iota(jnp.int32, (GROUP, LANES), 1)
    low_top = [(lane_id + h).astype(jnp.int16) for h in range(0, B, LANES)]
    high_top = [((lane_id + h) * B + (B - 1 - OFFSET)).astype(jnp.int16) for h in range(0, B, LANES)]
    one = jnp.ones((GROUP, LANES), jnp.bfloat16)
    none = jnp.zeros((GROUP, LANES), jnp.bfloat16)
    tiles = [(t, p) for t in range(shard // WIDE) for p in range(half)]

    def columns(blocks):
        parts = []
        for codes in blocks:
            wide = codes.astype(jnp.int32)
            parts.append(wide[:half] + wide[half:] * B - OFFSET)
        cols_ref[:, :half * len(blocks)] = jnp.concatenate(parts, axis=0).T.astype(jnp.int16)

    def spread(t, p, at):
        for row in range(t * WIDE, (t + 1) * WIDE, GROUP):
            tile_ref[p, row:row + GROUP] = jnp.broadcast_to(
                cols_ref[row:row + GROUP, at + p:at + p + 1], (GROUP, LANES))

    def weigh(where, t):
        for j in range(t * WIDE // LANES, (t + 1) * WIDE // LANES):
            start, _, end = spots(j)
            both = packed_all[where, start:end]
            node = packed_all[where, node_rows + j:node_rows + j + 1]
            zero = jnp.zeros_like(both)
            for leaf in range(LEAVES):
                lhs_ref[j, leaf * width:(leaf + 1) * width] = jnp.where(node == leaf, both, zero)

    def push(k):
        t, p = tiles[k % len(tiles)]
        low, high = [], []
        for row in range(t * WIDE, (t + 1) * WIDE, GROUP):
            code = tile_ref[p, row:row + GROUP]
            rest = code & (B - 1)
            low.append(jnp.concatenate([jnp.where(rest <= top, one, none) for top in low_top], axis=1))
            high.append(jnp.concatenate([jnp.where(code <= top, one, none) for top in high_top], axis=1))
        pltpu.matmul_push_rhs(jnp.concatenate(low, axis=0), k % 2, 0)
        pltpu.matmul_push_rhs(jnp.concatenate(high, axis=0), k % 2, 1)

    def add_block(later, at):
        for k, (t, p) in enumerate(tiles):
            if k + 1 < len(tiles):
                push(k + 1)
            span = range(t * WIDE // LANES, (t + 1) * WIDE // LANES)
            lhs = jnp.concatenate([lhs_ref[j] for j in span], axis=1)
            pltpu.matmul_acc_lhs(accs[p], lhs, load_staged_rhs=k % 2)
            pltpu.matmul_acc_lhs(accs[half + p], lhs, load_staged_rhs=k % 2)
            if later is not None:
                spread(t, p, at)
                if p == half - 1:
                    weigh(later, t)
        if later is not None:
            push(len(tiles))

    for acc in accs:
        pltpu.matmul_pop(acc)

    sent = []

    def packed_copy(slot, sem, where, part):
        rows = slice(cuts[part], cuts[part + 1])
        return pltpu.make_async_remote_copy(
            src_ref=packed_all.at[slot, rows], dst_ref=packed_all.at[slot, rows], send_sem=send_g.at[sem],
            recv_sem=recv_g.at[slot, part], device_id=where, device_id_type=MESH)

    def wait_packed(slot, part):
        packed_copy(slot, 0, beside_me, part).wait_recv()

    def send_packed(slot, where, part, when):
        sem = len(sent)
        sent.append((part, when))
        copy = packed_copy(slot, sem, where, part)
        pl.when(when())(copy.start)

    def beside_copy(slot, p):
        return pltpu.make_async_remote_copy(
            src_ref=packed_all.at[slot], dst_ref=packed_all.at[slot], send_sem=send_s.at[p],
            recv_sem=recv_g.at[slot, 0], device_id=beside_me, device_id_type=MESH)

    def send_codes(q, mine=True):
        da, db, dz = offsets(q, c)
        ta, tb, tz = lax.rem(a + na - da, na), lax.rem(b + nb - db, nb), toggled(dz)
        base = line(ta, tb, tz, 0)
        for k in range(0 if mine else 1, 2):
            pc = other if k else c
            pltpu.make_async_remote_copy(
                src_ref=codes_in.at[base + pc], dst_ref=codes_all.at[me], send_sem=send_c.at[2 * q + k],
                recv_sem=recv_c.at[me], device_id=place(ta, tb, tz, pc), device_id_type=MESH).start()

    def is_core(core):
        return c == core

    def passes(step, k):
        origin, there = z - step * k, z + step
        return jnp.logical_and(
            jnp.logical_and(origin >= 0, origin < nz), jnp.logical_and(there >= 0, there < nz))

    def in_plane(g, q, part):
        slot = source(g * group + q, c)
        for core in range(2):
            n1, n2 = (nb, na) if core == 0 else (na, nb)

            def spot(step, k):
                if (step == 1) == (core == 0):
                    return place(a, (b + nb - k) % nb, z, c)
                return place((a + na - k) % na, b, z, c)

            if q < n1:
                for k in range(1, n2):
                    send_packed(slot, spot(2, k), part, functools.partial(is_core, core))
            if q == 0:
                for k in range(1, n1):
                    send_packed(slot, spot(1, k), part, functools.partial(is_core, core))

    def along(k, part):
        for step in (1, -1):
            origin, there = z - step * k, z + step
            inside = jnp.logical_and(origin >= 0, origin < nz)
            slot = line(a, b, origin, c)
            if k > 0:
                @pl.when(inside)
                def _():
                    wait_packed(slot, part)
            send_packed(slot, place(a, b, there, c), part, functools.partial(passes, step, k))

    def relay(g, ahead):
        for part in range(PARTS):
            for q in range(1, early):
                wait_packed(source(g * group + q, c), part)
                in_plane(g, q, part)
            if ahead < nz:
                along(ahead, part)
                in_plane(ahead, 0, part)
        for q in range(1, early):
            beside_copy(source(g * group + q, c), g * group + q).start()
        if ahead < nz:
            beside_copy(source(ahead * group, c), ahead * group).start()

    def order(n):
        n = jnp.int32(n)
        at = lax.rem(n, group)
        ahead = jnp.logical_and(at == group - 1, n < pairs - 1)
        behind = jnp.logical_and(at == 0, n > 0)
        return n + jnp.where(ahead, 1, 0) - jnp.where(behind, 1, 0)

    early = max(na, nb)
    around = 2 * group - 1 + 2 * jnp.where(z > 0, 1, 0) + 2 * jnp.where(z + 1 < nz, 1, 0)

    loads[0].wait()
    node = jnp.concatenate(
        [leaf_in[...].astype(jnp.float32), jnp.zeros((nodes - chunks, LANES), jnp.float32)], axis=0)
    packed_all[me, node_rows:node_rows + nodes] = node.astype(jnp.bfloat16)
    for copy in loads[1:]:
        copy.wait()

    pl.semaphore_wait(barrier, around)

    for part in range(PARTS):
        along(0, part)
        in_plane(0, 0, part)
    beside_copy(me, 0).start()

    load_bins.wait()
    codes_in[...] = bins_in[...].astype(jnp.int16).reshape(codes_in.shape)
    for n in range(group + 1):
        send_codes(order(n), n > 0)

    def wait_codes(here):
        pltpu.make_async_remote_copy(
            src_ref=codes_all.at[here], dst_ref=codes_all.at[here], send_sem=send_c.at[0],
            recv_sem=recv_c.at[here], device_id=beside_me, device_id_type=MESH).wait_recv()

    def wait_beside(beside):
        wait_codes(beside)
        pltpu.make_async_remote_copy(
            src_ref=packed_all.at[beside], dst_ref=packed_all.at[beside], send_sem=send_s.at[0],
            recv_sem=recv_g.at[beside, 0], device_id=beside_me, device_id_type=MESH).wait_recv()

    columns([codes_in[me]])
    for t, p in tiles:
        spread(t, p, 0)
        if p == half - 1:
            weigh(me, t)
    push(0)

    beside = source(0, other)
    wait_beside(beside)
    columns([codes_all[beside]])
    add_block(beside, 0)
    relay(0, 1)
    later = source(order(1), c)
    wait_codes(later)
    columns([codes_all[later]])
    add_block(later, 0)

    def step(i, slots):
        beside, later = slots
        for g in range(nz - 1):
            @pl.when(i == (g + 1) * (group - 1))
            def _():
                relay(g + 1, g + 2)

        @pl.when(lax.rem(order(i + 1), group) >= early)
        def _():
            for part in range(PARTS):
                wait_packed(later, part)
            beside_copy(later, order(i + 1)).start()

        @pl.when(i + (group + 1) <= pairs)
        def _():
            send_codes(order(i + (group + 1) - 1))

        wait_beside(beside)
        wait_codes(later)
        columns([codes_all[beside], codes_all[later]])
        add_block(beside, 0)
        add_block(later, half)
        return source(order(i + 1), other), source(order(i + 2), c)

    beside, _ = lax.fori_loop(1, pairs - 1, step, (source(order(1), other), source(order(2), c)))
    wait_beside(beside)
    columns([codes_all[beside]])
    add_block(beside, 0)
    add_block(None, 0)

    top = None
    for i in range(owned):
        value = feature_gains(pltpu.matmul_pop(accs[i]), outputs)
        for h in range(B // LANES):
            row = (i * (B // LANES) + h) * LEAVES
            gains_ref[row:row + LEAVES] = value[:, h * LANES:(h + 1) * LANES]
        top = value if top is None else jnp.maximum(top, value)
    peak = jnp.max(top, axis=1, keepdims=True)
    lane = lax.broadcasted_iota(jnp.int32, (1, LANES), 1)
    best_all[me] = jnp.where(lane == 0, peak[0:1], peak[1:2])

    others = [(i, j) for i in range(group) for j in range(nz * 2) if i + j > 0]
    for i, j in reversed(others):
        pltpu.make_async_remote_copy(
            src_ref=best_all.at[me], dst_ref=best_all.at[me], send_sem=send_b, recv_sem=recv_b,
            device_id={"rows": lax.rem(r + i, group), "feat": lax.rem(f + j, nz * 2)},
            device_id_type=MESH).start()

    @pl.loop(1, count)
    def _(s):
        pltpu.make_async_remote_copy(
            src_ref=codes_in.at[0], dst_ref=codes_all.at[0], send_sem=send_c.at[s],
            recv_sem=recv_c.at[0], device_id=beside_me, device_id_type=MESH).wait_send()

    @pl.loop(0, pairs)
    def _(p):
        beside_copy(me, p).wait_send()

    for sem, (part, when) in enumerate(sent):
        pl.when(when())(packed_copy(me, sem, beside_me, part).wait_send)

    rest = best_all.at[0:count - 1]
    bests = pltpu.make_async_remote_copy(
        src_ref=rest, dst_ref=rest, send_sem=send_b, recv_sem=recv_b,
        device_id=beside_me, device_id_type=MESH)
    bests.wait_recv()
    bests.wait_send()

    best_ref[...] = jnp.max(best_all[...], axis=0)[:, :LEAVES]


def shards(sizes, bins, leaf, grad, hess):
    na, nb, nz = sizes
    count = na * nb * nz * 2
    outputs = grad.shape[0]
    features, shard = bins.shape
    owned = features // count
    chunks = shard // LANES
    packed_rows = chunks * 2 * outputs + chunks + -chunks % 16
    codes_shape = (count, owned, shard)
    halves = B // LANES
    gains, best = pl.pallas_call(
        functools.partial(kernel, sizes, outputs, shard, owned),
        out_shape=(
            pltpu.VMEM((owned * halves * LEAVES, LANES), jnp.float32),
            pltpu.VMEM((1, LEAVES), jnp.float32),
        ),
        in_specs=[pl.BlockSpec(memory_space=pl.ANY)] * 4,
        out_specs=(pl.BlockSpec(memory_space=pltpu.VMEM),) * 2,
        scratch_shapes=[
            pltpu.VMEM((features, shard), jnp.int32),
            pltpu.VMEM((chunks, LANES), jnp.int32),
            pltpu.VMEM(codes_shape, jnp.int16),
            pltpu.VMEM(codes_shape, jnp.int16),
            pltpu.VMEM((count, packed_rows, LANES), jnp.bfloat16),
            pltpu.VMEM((count, 1, LANES), jnp.float32),
        ],
        compiler_params=pltpu.CompilerParams(
            collective_id=0, has_side_effects=True, vmem_limit_bytes=56 * 1024 * 1024
        ),
    )(bins, leaf.reshape(chunks, LANES), grad, hess)
    gains = gains.reshape(owned, halves, LEAVES, LANES).transpose(0, 2, 1, 3).reshape(owned, LEAVES, B)
    return gains, best.reshape(LEAVES)


def solution(mesh):
    rows, feat = mesh.shape["rows"], mesh.shape["feat"]
    sizes = (rows // 2, 2, feat // 2)
    return jax.shard_map(
        functools.partial(shards, sizes),
        mesh=mesh,
        in_specs=(
            P(None, ("rows", "feat")),
            P(("rows", "feat")),
            P(None, ("rows", "feat")),
            P(None, ("rows", "feat")),
        ),
        out_specs=(P(("rows", "feat"), None, None), P()),
        check_vma=False,
    )
```

```python
import functools

import jax
import jax.numpy as jnp
from jax import lax
from jax.experimental import pallas as pl
from jax.experimental.pallas import tpu as pltpu
from jax.sharding import PartitionSpec as P

B = 256
LEAVES = 2
LANES = 128
WIDE = 256
GROUP = 16
OFFSET = 32768
PARTS = 2
MESH = pl.DeviceIdType.MESH


def accumulator(mxu, height):
    return pltpu.ACC(mxu)((height, B), jnp.float32)


def feature_gains(cum, outputs):
    rows = []
    for leaf in range(LEAVES):
        base = leaf * 2 * outputs
        left_grad = cum[base:base + outputs]
        left_hess = cum[base + outputs:base + 2 * outputs]
        all_grad = left_grad[:, B - 1:B]
        all_hess = left_hess[:, B - 1:B]
        right_grad = all_grad - left_grad
        right_hess = all_hess - left_hess
        score = (
            left_grad * left_grad / (left_hess + 1.0)
            + right_grad * right_grad / (right_hess + 1.0)
            - all_grad * all_grad / (all_hess + 1.0)
        )
        rows.append(0.5 / outputs * jnp.sum(score, axis=0, keepdims=True))
    return jnp.concatenate(rows, axis=0)


def kernel(sizes, outputs, shard, owned, *refs):
    na, nb, nz = sizes
    half = owned // 2
    height = LEAVES * 2 * outputs
    count = na * nb * nz * 2
    sends = PARTS * (2 * nz + 2 * nz * max(na, nb) * (na + nb))
    dma = pltpu.SemaphoreType.DMA((count,))
    one = pltpu.SemaphoreType.DMA
    pl.run_scoped(
        functools.partial(body, sizes, outputs, shard, owned, refs),
        *[accumulator(0, height)] * half,
        *[accumulator(1, height)] * half,
        pltpu.VMEM((shard // LANES, height, LANES), jnp.bfloat16),
        pltpu.VMEM((half, shard, LANES), jnp.int16),
        pltpu.VMEM((shard, owned), jnp.int16),
        pltpu.SemaphoreType.DMA((2 * shard // LANES + 2,)),
        dma, dma,
        pltpu.SemaphoreType.DMA((sends,)),
        pltpu.SemaphoreType.DMA((count, PARTS)),
        dma, one, one,
    )


def body(sizes, outputs, shard, owned, refs, *scoped):
    (bins_ref, leaf_ref, grad_ref, hess_ref, gains_ref, best_ref,
     bins_in, leaf_in, codes_in, codes_all, packed_all, best_all) = refs
    accs = scoped[:owned]
    (lhs_ref, tile_ref, cols_ref,
     load, send_c, recv_c, send_g, recv_g, send_s, send_b, recv_b) = scoped[owned:]
    na, nb, nz = sizes
    group = na * nb
    pairs = group * nz
    count = 2 * pairs
    chunks = shard // LANES
    half = owned // 2
    width = 2 * outputs
    nodes = chunks + -chunks % 16
    r = lax.axis_index("rows")
    f = lax.axis_index("feat")
    a, b = r // nb, r % nb
    z, c = f // 2, f % 2
    other = 1 - c

    def place(pa, pb, pz, pc):
        return {"rows": pa * nb + pb, "feat": pz * 2 + pc}

    def line(pa, pb, pz, pc):
        return ((pa * nb + pb) * nz + pz) * 2 + pc

    def toggled(dz):
        value, bit = 0, 1
        while bit < nz:
            value = value + lax.rem(lax.div(z, bit) + lax.div(dz, bit), 2) * bit
            bit *= 2
        return value

    def offsets(p, pc):
        p = jnp.int32(p)
        da = (1 - pc) * lax.rem(lax.div(p, nb), na) + pc * lax.rem(p, na)
        db = (1 - pc) * lax.rem(p, nb) + pc * lax.rem(lax.div(p, na), nb)
        return da, db, lax.div(p, group)

    me = line(a, b, z, c)
    beside_me = place(a, b, z, other)

    def source(p, pc):
        da, db, dz = offsets(p, pc)
        return line(lax.rem(a + da, na), lax.rem(b + db, nb), toggled(dz), pc)

    barrier = pltpu.get_barrier_semaphore()

    def greet(where):
        pl.semaphore_signal(barrier, inc=1, device_id=where, device_id_type=MESH)

    for step in (1, -1):
        @pl.when(jnp.logical_and(z + step >= 0, z + step < nz))
        def _():
            for pc in range(2):
                greet(place(a, b, z + step, pc))
    for i in range(na):
        for j in range(nb):
            for k in range(2):
                if i + j + k > 0:
                    greet(place((a + i) % na, (b + j) % nb, z, (c + k) % 2))

    def spots(j):
        start = j * width + (j >= chunks // PARTS) * nodes
        return start, start + outputs, start + width

    node_rows = chunks // PARTS * width
    cuts = [0] + [k * (chunks // PARTS) * width + nodes for k in range(1, PARTS + 1)]
    loads = [pltpu.make_async_copy(leaf_ref, leaf_in, load.at[2 * chunks])]
    for j in range(chunks):
        part = slice(j * LANES, (j + 1) * LANES)
        start, middle, end = spots(j)
        loads.append(pltpu.make_async_copy(
            grad_ref.at[:, part], packed_all.at[me, start:middle], load.at[2 * j]))
        loads.append(pltpu.make_async_copy(
            hess_ref.at[:, part], packed_all.at[me, middle:end], load.at[2 * j + 1]))
    load_bins = pltpu.make_async_copy(bins_ref, bins_in, load.at[2 * chunks + 1])
    for copy in loads:
        copy.start()
    load_bins.start()

    lane_id = lax.broadcasted_iota(jnp.int32, (GROUP, LANES), 1)
    low_top = [(lane_id + h).astype(jnp.int16) for h in range(0, B, LANES)]
    high_top = [((lane_id + h) * B + (B - 1 - OFFSET)).astype(jnp.int16) for h in range(0, B, LANES)]
    one = jnp.ones((GROUP, LANES), jnp.bfloat16)
    none = jnp.zeros((GROUP, LANES), jnp.bfloat16)
    tiles = [(t, p) for t in range(shard // WIDE) for p in range(half)]

    def columns(blocks):
        parts = []
        for codes in blocks:
            wide = codes.astype(jnp.int32)
            parts.append(wide[:half] + wide[half:] * B - OFFSET)
        cols_ref[:, :half * len(blocks)] = jnp.concatenate(parts, axis=0).T.astype(jnp.int16)

    def spread(t, p, at):
        for row in range(t * WIDE, (t + 1) * WIDE, GROUP):
            tile_ref[p, row:row + GROUP] = jnp.broadcast_to(
                cols_ref[row:row + GROUP, at + p:at + p + 1], (GROUP, LANES))

    def weigh(where, t):
        for j in range(t * WIDE // LANES, (t + 1) * WIDE // LANES):
            start, _, end = spots(j)
            both = packed_all[where, start:end]
            node = packed_all[where, node_rows + j:node_rows + j + 1]
            zero = jnp.zeros_like(both)
            for leaf in range(LEAVES):
                lhs_ref[j, leaf * width:(leaf + 1) * width] = jnp.where(node == leaf, both, zero)

    def push(k, tiles=tiles):
        t, p = tiles[k % len(tiles)]
        low, high = [], []
        for row in range(t * WIDE, (t + 1) * WIDE, GROUP):
            code = tile_ref[p, row:row + GROUP]
            rest = code & (B - 1)
            low.append(jnp.concatenate([jnp.where(rest <= top, one, none) for top in low_top], axis=1))
            high.append(jnp.concatenate([jnp.where(code <= top, one, none) for top in high_top], axis=1))
        pltpu.matmul_push_rhs(jnp.concatenate(low, axis=0), k % 2, 0)
        pltpu.matmul_push_rhs(jnp.concatenate(high, axis=0), k % 2, 1)

    def multiply(k, t, p):
        span = range(t * WIDE // LANES, (t + 1) * WIDE // LANES)
        lhs = jnp.concatenate([lhs_ref[j] for j in span], axis=1)
        pltpu.matmul_acc_lhs(accs[p], lhs, load_staged_rhs=k % 2)
        pltpu.matmul_acc_lhs(accs[half + p], lhs, load_staged_rhs=k % 2)

    def add_block(later, at):
        for k, (t, p) in enumerate(tiles):
            if k + 1 < len(tiles):
                push(k + 1)
            multiply(k, t, p)
            spread(t, p, at)
            if p == half - 1:
                weigh(later, t)
        push(len(tiles))

    for acc in accs:
        pltpu.matmul_pop(acc)

    sent = []

    def packed_copy(slot, sem, where, part):
        rows = slice(cuts[part], cuts[part + 1])
        return pltpu.make_async_remote_copy(
            src_ref=packed_all.at[slot, rows], dst_ref=packed_all.at[slot, rows], send_sem=send_g.at[sem],
            recv_sem=recv_g.at[slot, part], device_id=where, device_id_type=MESH)

    def wait_packed(slot, part):
        packed_copy(slot, 0, beside_me, part).wait_recv()

    def send_packed(slot, where, part, when):
        sem = len(sent)
        sent.append((part, when))
        copy = packed_copy(slot, sem, where, part)
        pl.when(when())(copy.start)

    def beside_copy(slot, p):
        return pltpu.make_async_remote_copy(
            src_ref=packed_all.at[slot], dst_ref=packed_all.at[slot], send_sem=send_s.at[p],
            recv_sem=recv_g.at[slot, 0], device_id=beside_me, device_id_type=MESH)

    def send_codes(q, mine=True):
        da, db, dz = offsets(q, c)
        ta, tb, tz = lax.rem(a + na - da, na), lax.rem(b + nb - db, nb), toggled(dz)
        base = line(ta, tb, tz, 0)
        for k in range(0 if mine else 1, 2):
            pc = other if k else c
            pltpu.make_async_remote_copy(
                src_ref=codes_in.at[base + pc], dst_ref=codes_all.at[me], send_sem=send_c.at[2 * q + k],
                recv_sem=recv_c.at[me], device_id=place(ta, tb, tz, pc), device_id_type=MESH).start()

    def is_core(core):
        return c == core

    def passes(step, k):
        origin, there = z - step * k, z + step
        return jnp.logical_and(
            jnp.logical_and(origin >= 0, origin < nz), jnp.logical_and(there >= 0, there < nz))

    def in_plane(g, q, part):
        slot = source(g * group + q, c)
        for core in range(2):
            n1, n2 = (nb, na) if core == 0 else (na, nb)

            def spot(step, k):
                if (step == 1) == (core == 0):
                    return place(a, (b + nb - k) % nb, z, c)
                return place((a + na - k) % na, b, z, c)

            if q < n1:
                for k in range(1, n2):
                    send_packed(slot, spot(2, k), part, functools.partial(is_core, core))
            if q == 0:
                for k in range(1, n1):
                    send_packed(slot, spot(1, k), part, functools.partial(is_core, core))

    def along(k, part):
        for step in (1, -1):
            origin, there = z - step * k, z + step
            inside = jnp.logical_and(origin >= 0, origin < nz)
            slot = line(a, b, origin, c)
            if k > 0:
                @pl.when(inside)
                def _():
                    wait_packed(slot, part)
            send_packed(slot, place(a, b, there, c), part, functools.partial(passes, step, k))

    def relay(g, ahead):
        for part in range(PARTS):
            if ahead < nz:
                along(ahead, part)
            for q in range(1, early):
                wait_packed(source(g * group + q, c), part)
                in_plane(g, q, part)
            if ahead < nz:
                in_plane(ahead, 0, part)
        for q in range(1, early):
            beside_copy(source(g * group + q, c), g * group + q).start()
        if ahead < nz:
            beside_copy(source(ahead * group, c), ahead * group).start()

    def order(n):
        n = jnp.int32(n)
        at = lax.rem(n, group)
        ahead = jnp.logical_and(at == group - 1, n < pairs - 1)
        behind = jnp.logical_and(at == 0, n > 0)
        return n + jnp.where(ahead, 1, 0) - jnp.where(behind, 1, 0)

    early = max(na, nb)
    around = 2 * group - 1 + 2 * jnp.where(z > 0, 1, 0) + 2 * jnp.where(z + 1 < nz, 1, 0)

    loads[0].wait()
    node = jnp.concatenate(
        [leaf_in[...].astype(jnp.float32), jnp.zeros((nodes - chunks, LANES), jnp.float32)], axis=0)
    packed_all[me, node_rows:node_rows + nodes] = node.astype(jnp.bfloat16)
    for copy in loads[1:]:
        copy.wait()

    pl.semaphore_wait(barrier, around)

    for part in range(PARTS):
        along(0, part)
        in_plane(0, 0, part)
    beside_copy(me, 0).start()

    load_bins.wait()
    codes_in[...] = bins_in[...].astype(jnp.int16).reshape(codes_in.shape)
    for n in range(group + 1):
        send_codes(order(n), n > 0)

    def wait_codes(here):
        pltpu.make_async_remote_copy(
            src_ref=codes_all.at[here], dst_ref=codes_all.at[here], send_sem=send_c.at[0],
            recv_sem=recv_c.at[here], device_id=beside_me, device_id_type=MESH).wait_recv()

    def wait_beside(beside):
        wait_codes(beside)
        pltpu.make_async_remote_copy(
            src_ref=packed_all.at[beside], dst_ref=packed_all.at[beside], send_sem=send_s.at[0],
            recv_sem=recv_g.at[beside, 0], device_id=beside_me, device_id_type=MESH).wait_recv()

    columns([codes_in[me]])
    for t, p in tiles:
        spread(t, p, 0)
        if p == half - 1:
            weigh(me, t)
    push(0)

    beside = source(0, other)
    wait_beside(beside)
    columns([codes_all[beside]])
    add_block(beside, 0)
    relay(0, 1)
    send_codes(order(group + 1))
    later = source(order(1), c)
    wait_codes(later)
    columns([codes_all[later]])
    add_block(later, 0)

    first = group + 2

    def step(sending, start, stop, i, slots):
        beside, later = slots
        for g in range(nz - 1):
            if not start <= (g + 1) * (group - 1) < stop:
                continue

            @pl.when(i == (g + 1) * (group - 1))
            def _():
                relay(g + 1, g + 2)

        @pl.when(lax.rem(order(i + 1), group) >= early)
        def _():
            for part in range(PARTS):
                wait_packed(later, part)
            beside_copy(later, order(i + 1)).start()

        wait_beside(beside)
        wait_codes(later)
        columns([codes_all[beside], codes_all[later]])
        add_block(beside, 0)
        if sending:
            send_codes(order(i + first - 1))
        add_block(later, half)
        return source(order(i + 1), other), source(order(i + 2), c)

    slots = source(order(1), other), source(order(2), c)
    for sending, start, stop in ((True, 1, pairs - first + 1), (False, pairs - first + 1, pairs - 1)):
        slots = lax.fori_loop(start, stop, functools.partial(step, sending, start, stop), slots)
    beside = slots[0]
    wait_beside(beside)
    columns([codes_all[beside]])
    add_block(beside, 0)
    finals = [(t, p) for p in range(half) for t in range(shard // WIDE)]
    top = None
    for k, (t, p) in enumerate(finals):
        if k + 1 < len(finals):
            push(k + 1, finals)
        multiply(k, t, p)
        if t == shard // WIDE - 1:
            for i in (p, half + p):
                value = feature_gains(pltpu.matmul_pop(accs[i]), outputs)
                for h in range(B // LANES):
                    row = (i * (B // LANES) + h) * LEAVES
                    gains_ref[row:row + LEAVES] = value[:, h * LANES:(h + 1) * LANES]
                top = value if top is None else jnp.maximum(top, value)
    peak = jnp.max(top, axis=1, keepdims=True)
    lane = lax.broadcasted_iota(jnp.int32, (1, LANES), 1)
    best_all[me] = jnp.where(lane == 0, peak[0:1], peak[1:2])

    others = [(i, j) for i in range(group) for j in range(nz * 2) if i + j > 0]
    for i, j in reversed(others):
        pltpu.make_async_remote_copy(
            src_ref=best_all.at[me], dst_ref=best_all.at[me], send_sem=send_b, recv_sem=recv_b,
            device_id={"rows": lax.rem(r + i, group), "feat": lax.rem(f + j, nz * 2)},
            device_id_type=MESH).start()

    @pl.loop(1, count)
    def _(s):
        pltpu.make_async_remote_copy(
            src_ref=codes_in.at[0], dst_ref=codes_all.at[0], send_sem=send_c.at[s],
            recv_sem=recv_c.at[0], device_id=beside_me, device_id_type=MESH).wait_send()

    @pl.loop(0, pairs)
    def _(p):
        beside_copy(me, p).wait_send()

    for sem, (part, when) in enumerate(sent):
        pl.when(when())(packed_copy(me, sem, beside_me, part).wait_send)

    rest = best_all.at[0:count - 1]
    bests = pltpu.make_async_remote_copy(
        src_ref=rest, dst_ref=rest, send_sem=send_b, recv_sem=recv_b,
        device_id=beside_me, device_id_type=MESH)
    bests.wait_recv()
    bests.wait_send()

    best_ref[...] = jnp.max(best_all[...], axis=0)[:, :LEAVES]


def shards(sizes, bins, leaf, grad, hess):
    na, nb, nz = sizes
    count = na * nb * nz * 2
    outputs = grad.shape[0]
    features, shard = bins.shape
    owned = features // count
    chunks = shard // LANES
    packed_rows = chunks * 2 * outputs + chunks + -chunks % 16
    codes_shape = (count, owned, shard)
    halves = B // LANES
    gains, best = pl.pallas_call(
        functools.partial(kernel, sizes, outputs, shard, owned),
        out_shape=(
            pltpu.VMEM((owned * halves * LEAVES, LANES), jnp.float32),
            pltpu.VMEM((1, LEAVES), jnp.float32),
        ),
        in_specs=[pl.BlockSpec(memory_space=pl.ANY)] * 4,
        out_specs=(pl.BlockSpec(memory_space=pltpu.VMEM),) * 2,
        scratch_shapes=[
            pltpu.VMEM((features, shard), jnp.int32),
            pltpu.VMEM((chunks, LANES), jnp.int32),
            pltpu.VMEM(codes_shape, jnp.int16),
            pltpu.VMEM(codes_shape, jnp.int16),
            pltpu.VMEM((count, packed_rows, LANES), jnp.bfloat16),
            pltpu.VMEM((count, 1, LANES), jnp.float32),
        ],
        compiler_params=pltpu.CompilerParams(
            collective_id=0, has_side_effects=True, vmem_limit_bytes=56 * 1024 * 1024
        ),
    )(bins, leaf.reshape(chunks, LANES), grad, hess)
    gains = gains.reshape(owned, halves, LEAVES, LANES).transpose(0, 2, 1, 3).reshape(owned, LEAVES, B)
    return gains, best.reshape(LEAVES)


def solution(mesh):
    rows, feat = mesh.shape["rows"], mesh.shape["feat"]
    sizes = (rows // 2, 2, feat // 2)
    return jax.shard_map(
        functools.partial(shards, sizes),
        mesh=mesh,
        in_specs=(
            P(None, ("rows", "feat")),
            P(("rows", "feat")),
            P(None, ("rows", "feat")),
            P(None, ("rows", "feat")),
        ),
        out_specs=(P(("rows", "feat"), None, None), P()),
        check_vma=False,
    )
```

```python
import functools

import jax
import jax.numpy as jnp
from jax import lax
from jax.experimental import pallas as pl
from jax.experimental.pallas import tpu as pltpu
from jax.sharding import PartitionSpec as P

B = 256
LEAVES = 2
LANES = 128
WIDE = 256
GROUP = 16
OFFSET = 32768
PARTS = 2
MESH = pl.DeviceIdType.MESH


def accumulator(mxu, height):
    return pltpu.ACC(mxu)((height, B), jnp.float32)


def feature_gains(cum, outputs):
    rows = []
    for leaf in range(LEAVES):
        base = leaf * 2 * outputs
        left_grad = cum[base:base + outputs]
        left_hess = cum[base + outputs:base + 2 * outputs]
        all_grad = left_grad[:, B - 1:B]
        all_hess = left_hess[:, B - 1:B]
        right_grad = all_grad - left_grad
        right_hess = all_hess - left_hess
        score = (
            left_grad * left_grad / (left_hess + 1.0)
            + right_grad * right_grad / (right_hess + 1.0)
            - all_grad * all_grad / (all_hess + 1.0)
        )
        rows.append(0.5 / outputs * jnp.sum(score, axis=0, keepdims=True))
    return jnp.concatenate(rows, axis=0)


def kernel(sizes, outputs, shard, owned, *refs):
    na, nb, nz = sizes
    half = owned // 2
    height = LEAVES * 2 * outputs
    count = na * nb * nz * 2
    sends = PARTS * (2 * nz + 2 * nz * max(na, nb) * (na + nb))
    dma = pltpu.SemaphoreType.DMA((count,))
    one = pltpu.SemaphoreType.DMA
    pl.run_scoped(
        functools.partial(body, sizes, outputs, shard, owned, refs),
        *[accumulator(0, height)] * half,
        *[accumulator(1, height)] * half,
        pltpu.VMEM((shard // LANES, height, LANES), jnp.bfloat16),
        pltpu.VMEM((half, shard, LANES), jnp.int16),
        pltpu.VMEM((shard, owned), jnp.int16),
        pltpu.SemaphoreType.DMA((2 * shard // LANES + 2,)),
        dma, dma,
        pltpu.SemaphoreType.DMA((sends,)),
        pltpu.SemaphoreType.DMA((count, PARTS)),
        dma, one, one,
    )


def body(sizes, outputs, shard, owned, refs, *scoped):
    (bins_ref, leaf_ref, grad_ref, hess_ref, gains_ref, best_ref,
     bins_in, leaf_in, codes_in, codes_all, packed_all, best_all) = refs
    accs = scoped[:owned]
    (lhs_ref, tile_ref, cols_ref,
     load, send_c, recv_c, send_g, recv_g, send_s, send_b, recv_b) = scoped[owned:]
    na, nb, nz = sizes
    group = na * nb
    pairs = group * nz
    count = 2 * pairs
    chunks = shard // LANES
    half = owned // 2
    width = 2 * outputs
    nodes = chunks + -chunks % 16
    r = lax.axis_index("rows")
    f = lax.axis_index("feat")
    a, b = r // nb, r % nb
    z, c = f // 2, f % 2
    other = 1 - c

    def place(pa, pb, pz, pc):
        return {"rows": pa * nb + pb, "feat": pz * 2 + pc}

    def line(pa, pb, pz, pc):
        return ((pa * nb + pb) * nz + pz) * 2 + pc

    def toggled(dz):
        value, bit = 0, 1
        while bit < nz:
            value = value + lax.rem(lax.div(z, bit) + lax.div(dz, bit), 2) * bit
            bit *= 2
        return value

    def offsets(p, pc):
        p = jnp.int32(p)
        da = (1 - pc) * lax.rem(lax.div(p, nb), na) + pc * lax.rem(p, na)
        db = (1 - pc) * lax.rem(p, nb) + pc * lax.rem(lax.div(p, na), nb)
        return da, db, lax.div(p, group)

    me = line(a, b, z, c)
    beside_me = place(a, b, z, other)

    def source(p, pc):
        da, db, dz = offsets(p, pc)
        return line(lax.rem(a + da, na), lax.rem(b + db, nb), toggled(dz), pc)

    barrier = pltpu.get_barrier_semaphore()

    def greet(where):
        pl.semaphore_signal(barrier, inc=1, device_id=where, device_id_type=MESH)

    for step in (1, -1):
        @pl.when(jnp.logical_and(z + step >= 0, z + step < nz))
        def _():
            for pc in range(2):
                greet(place(a, b, z + step, pc))
    for i in range(na):
        for j in range(nb):
            for k in range(2):
                if i + j + k > 0:
                    greet(place((a + i) % na, (b + j) % nb, z, (c + k) % 2))

    def spots(j):
        start = j * width + (j >= chunks // PARTS) * nodes
        return start, start + outputs, start + width

    node_rows = chunks // PARTS * width
    cuts = [0] + [k * (chunks // PARTS) * width + nodes for k in range(1, PARTS + 1)]
    loads = [pltpu.make_async_copy(leaf_ref, leaf_in, load.at[2 * chunks])]
    for j in range(chunks):
        part = slice(j * LANES, (j + 1) * LANES)
        start, middle, end = spots(j)
        loads.append(pltpu.make_async_copy(
            grad_ref.at[:, part], packed_all.at[me, start:middle], load.at[2 * j]))
        loads.append(pltpu.make_async_copy(
            hess_ref.at[:, part], packed_all.at[me, middle:end], load.at[2 * j + 1]))
    load_bins = pltpu.make_async_copy(bins_ref, bins_in, load.at[2 * chunks + 1])
    for copy in loads:
        copy.start()
    load_bins.start()

    lane_id = lax.broadcasted_iota(jnp.int32, (GROUP, LANES), 1)
    low_top = [(lane_id + h).astype(jnp.int16) for h in range(0, B, LANES)]
    high_top = [((lane_id + h) * B + (B - 1 - OFFSET)).astype(jnp.int16) for h in range(0, B, LANES)]
    one = jnp.ones((GROUP, LANES), jnp.bfloat16)
    none = jnp.zeros((GROUP, LANES), jnp.bfloat16)
    tiles = [(t, p) for t in range(shard // WIDE) for p in range(half)]

    def columns(blocks):
        parts = []
        for codes in blocks:
            wide = codes.astype(jnp.int32)
            parts.append(wide[:half] + wide[half:] * B - OFFSET)
        cols_ref[:, :half * len(blocks)] = jnp.concatenate(parts, axis=0).T.astype(jnp.int16)

    def spread(t, p, at):
        for row in range(t * WIDE, (t + 1) * WIDE, GROUP):
            tile_ref[p, row:row + GROUP] = jnp.broadcast_to(
                cols_ref[row:row + GROUP, at + p:at + p + 1], (GROUP, LANES))

    def weigh(where, t):
        for j in range(t * WIDE // LANES, (t + 1) * WIDE // LANES):
            start, _, end = spots(j)
            both = packed_all[where, start:end]
            node = packed_all[where, node_rows + j:node_rows + j + 1]
            zero = jnp.zeros_like(both)
            for leaf in range(LEAVES):
                lhs_ref[j, leaf * width:(leaf + 1) * width] = jnp.where(node == leaf, both, zero)

    def push(k, tiles=tiles):
        t, p = tiles[k % len(tiles)]
        low, high = [], []
        for row in range(t * WIDE, (t + 1) * WIDE, GROUP):
            code = tile_ref[p, row:row + GROUP]
            rest = code & (B - 1)
            low.append(jnp.concatenate([jnp.where(rest <= top, one, none) for top in low_top], axis=1))
            high.append(jnp.concatenate([jnp.where(code <= top, one, none) for top in high_top], axis=1))
        pltpu.matmul_push_rhs(jnp.concatenate(low, axis=0), k % 2, 0)
        pltpu.matmul_push_rhs(jnp.concatenate(high, axis=0), k % 2, 1)

    def multiply(k, t, p):
        span = range(t * WIDE // LANES, (t + 1) * WIDE // LANES)
        lhs = jnp.concatenate([lhs_ref[j] for j in span], axis=1)
        pltpu.matmul_acc_lhs(accs[p], lhs, load_staged_rhs=k % 2)
        pltpu.matmul_acc_lhs(accs[half + p], lhs, load_staged_rhs=k % 2)

    def add_block(later, at):
        for k, (t, p) in enumerate(tiles):
            if k + 1 < len(tiles):
                push(k + 1)
            multiply(k, t, p)
            spread(t, p, at)
            if p == half - 1:
                weigh(later, t)
        push(len(tiles))

    sent = []

    def packed_copy(slot, sem, where, part):
        rows = slice(cuts[part], cuts[part + 1])
        return pltpu.make_async_remote_copy(
            src_ref=packed_all.at[slot, rows], dst_ref=packed_all.at[slot, rows], send_sem=send_g.at[sem],
            recv_sem=recv_g.at[slot, part], device_id=where, device_id_type=MESH)

    def wait_packed(slot, part):
        packed_copy(slot, 0, beside_me, part).wait_recv()

    def send_packed(slot, where, part, when):
        sem = len(sent)
        sent.append((part, when))
        copy = packed_copy(slot, sem, where, part)
        pl.when(when())(copy.start)

    def beside_copy(slot, p):
        return pltpu.make_async_remote_copy(
            src_ref=packed_all.at[slot], dst_ref=packed_all.at[slot], send_sem=send_s.at[p],
            recv_sem=recv_g.at[slot, 0], device_id=beside_me, device_id_type=MESH)

    def send_codes(q, mine=True):
        da, db, dz = offsets(q, c)
        ta, tb, tz = lax.rem(a + na - da, na), lax.rem(b + nb - db, nb), toggled(dz)
        base = line(ta, tb, tz, 0)
        for k in range(0 if mine else 1, 2):
            pc = other if k else c
            pltpu.make_async_remote_copy(
                src_ref=codes_in.at[base + pc], dst_ref=codes_all.at[me], send_sem=send_c.at[2 * q + k],
                recv_sem=recv_c.at[me], device_id=place(ta, tb, tz, pc), device_id_type=MESH).start()

    def is_core(core):
        return c == core

    def passes(step, k):
        origin, there = z - step * k, z + step
        return jnp.logical_and(
            jnp.logical_and(origin >= 0, origin < nz), jnp.logical_and(there >= 0, there < nz))

    def in_plane(g, q, part):
        slot = source(g * group + q, c)
        for core in range(2):
            n1, n2 = (nb, na) if core == 0 else (na, nb)

            def spot(step, k):
                if (step == 1) == (core == 0):
                    return place(a, (b + nb - k) % nb, z, c)
                return place((a + na - k) % na, b, z, c)

            if q < n1:
                for k in range(1, n2):
                    send_packed(slot, spot(2, k), part, functools.partial(is_core, core))
            if q == 0:
                for k in range(1, n1):
                    send_packed(slot, spot(1, k), part, functools.partial(is_core, core))

    def along(k, part):
        for step in (1, -1):
            origin, there = z - step * k, z + step
            inside = jnp.logical_and(origin >= 0, origin < nz)
            slot = line(a, b, origin, c)
            if k > 0:
                @pl.when(inside)
                def _():
                    wait_packed(slot, part)
            send_packed(slot, place(a, b, there, c), part, functools.partial(passes, step, k))

    def relay(g, ahead):
        for part in range(PARTS):
            if ahead < nz:
                along(ahead, part)
            for q in range(1, early):
                wait_packed(source(g * group + q, c), part)
                in_plane(g, q, part)
            if ahead < nz:
                in_plane(ahead, 0, part)
        for q in range(1, early):
            beside_copy(source(g * group + q, c), g * group + q).start()
        if ahead < nz:
            beside_copy(source(ahead * group, c), ahead * group).start()

    def order(n):
        n = jnp.int32(n)
        at = lax.rem(n, group)
        ahead = jnp.logical_and(at == group - 1, n < pairs - 1)
        behind = jnp.logical_and(at == 0, n > 0)
        return n + jnp.where(ahead, 1, 0) - jnp.where(behind, 1, 0)

    early = max(na, nb)
    around = 2 * group - 1 + 2 * jnp.where(z > 0, 1, 0) + 2 * jnp.where(z + 1 < nz, 1, 0)

    loads[0].wait()
    node = jnp.concatenate(
        [leaf_in[...].astype(jnp.float32), jnp.zeros((nodes - chunks, LANES), jnp.float32)], axis=0)
    packed_all[me, node_rows:node_rows + nodes] = node.astype(jnp.bfloat16)
    for copy in loads[1:]:
        copy.wait()

    pl.semaphore_wait(barrier, around)

    for part in range(PARTS):
        along(0, part)
        in_plane(0, 0, part)
    beside_copy(me, 0).start()

    for acc in accs:
        pltpu.matmul_pop(acc)

    load_bins.wait()
    codes_in[...] = bins_in[...].astype(jnp.int16).reshape(codes_in.shape)
    for n in range(group + 1):
        send_codes(order(n), n > 0)

    def wait_codes(here):
        pltpu.make_async_remote_copy(
            src_ref=codes_all.at[here], dst_ref=codes_all.at[here], send_sem=send_c.at[0],
            recv_sem=recv_c.at[here], device_id=beside_me, device_id_type=MESH).wait_recv()

    def wait_beside(beside):
        wait_codes(beside)
        pltpu.make_async_remote_copy(
            src_ref=packed_all.at[beside], dst_ref=packed_all.at[beside], send_sem=send_s.at[0],
            recv_sem=recv_g.at[beside, 0], device_id=beside_me, device_id_type=MESH).wait_recv()

    columns([codes_in[me]])
    for t, p in tiles:
        spread(t, p, 0)
        if p == half - 1:
            weigh(me, t)
    push(0)

    beside = source(0, other)
    wait_beside(beside)
    columns([codes_all[beside]])
    add_block(beside, 0)
    relay(0, 1)
    send_codes(order(group + 1))
    later = source(order(1), c)
    wait_codes(later)
    columns([codes_all[later]])
    add_block(later, 0)

    first = group + 2

    def step(sending, start, stop, i, slots):
        beside, later = slots
        for g in range(nz - 1):
            if not start <= (g + 1) * (group - 1) < stop:
                continue

            @pl.when(i == (g + 1) * (group - 1))
            def _():
                relay(g + 1, g + 2)

        @pl.when(lax.rem(order(i + 1), group) >= early)
        def _():
            for part in range(PARTS):
                wait_packed(later, part)
            beside_copy(later, order(i + 1)).start()

        wait_beside(beside)
        wait_codes(later)
        columns([codes_all[beside], codes_all[later]])
        add_block(beside, 0)
        if sending:
            send_codes(order(i + first - 1))
        add_block(later, half)
        return source(order(i + 1), other), source(order(i + 2), c)

    slots = source(order(1), other), source(order(2), c)
    for sending, start, stop in ((True, 1, pairs - first + 1), (False, pairs - first + 1, pairs - 1)):
        slots = lax.fori_loop(start, stop, functools.partial(step, sending, start, stop), slots)
    beside = slots[0]
    wait_beside(beside)
    columns([codes_all[beside]])
    add_block(beside, 0)
    finals = [(t, p) for p in range(half) for t in range(shard // WIDE)]
    top = None
    for k, (t, p) in enumerate(finals):
        if k + 1 < len(finals):
            push(k + 1, finals)
        multiply(k, t, p)
        if t == shard // WIDE - 1:
            for i in (p, half + p):
                value = feature_gains(pltpu.matmul_pop(accs[i]), outputs)
                for h in range(B // LANES):
                    row = (i * (B // LANES) + h) * LEAVES
                    gains_ref[row:row + LEAVES] = value[:, h * LANES:(h + 1) * LANES]
                top = value if top is None else jnp.maximum(top, value)
    peak = jnp.max(top, axis=1, keepdims=True)
    lane = lax.broadcasted_iota(jnp.int32, (1, LANES), 1)
    best_all[me] = jnp.where(lane == 0, peak[0:1], peak[1:2])

    others = [(i, j) for i in range(group) for j in range(nz * 2) if i + j > 0]
    for i, j in reversed(others):
        pltpu.make_async_remote_copy(
            src_ref=best_all.at[me], dst_ref=best_all.at[me], send_sem=send_b, recv_sem=recv_b,
            device_id={"rows": lax.rem(r + i, group), "feat": lax.rem(f + j, nz * 2)},
            device_id_type=MESH).start()

    @pl.loop(1, count)
    def _(s):
        pltpu.make_async_remote_copy(
            src_ref=codes_in.at[0], dst_ref=codes_all.at[0], send_sem=send_c.at[s],
            recv_sem=recv_c.at[0], device_id=beside_me, device_id_type=MESH).wait_send()

    @pl.loop(0, pairs)
    def _(p):
        beside_copy(me, p).wait_send()

    for sem, (part, when) in enumerate(sent):
        pl.when(when())(packed_copy(me, sem, beside_me, part).wait_send)

    rest = best_all.at[0:count - 1]
    bests = pltpu.make_async_remote_copy(
        src_ref=rest, dst_ref=rest, send_sem=send_b, recv_sem=recv_b,
        device_id=beside_me, device_id_type=MESH)
    bests.wait_recv()
    bests.wait_send()

    best_ref[...] = jnp.max(best_all[...], axis=0)[:, :LEAVES]


def shards(sizes, bins, leaf, grad, hess):
    na, nb, nz = sizes
    count = na * nb * nz * 2
    outputs = grad.shape[0]
    features, shard = bins.shape
    owned = features // count
    chunks = shard // LANES
    packed_rows = chunks * 2 * outputs + chunks + -chunks % 16
    codes_shape = (count, owned, shard)
    halves = B // LANES
    gains, best = pl.pallas_call(
        functools.partial(kernel, sizes, outputs, shard, owned),
        out_shape=(
            pltpu.VMEM((owned * halves * LEAVES, LANES), jnp.float32),
            pltpu.VMEM((1, LEAVES), jnp.float32),
        ),
        in_specs=[pl.BlockSpec(memory_space=pl.ANY)] * 4,
        out_specs=(pl.BlockSpec(memory_space=pltpu.VMEM),) * 2,
        scratch_shapes=[
            pltpu.VMEM((features, shard), jnp.int32),
            pltpu.VMEM((chunks, LANES), jnp.int32),
            pltpu.VMEM(codes_shape, jnp.int16),
            pltpu.VMEM(codes_shape, jnp.int16),
            pltpu.VMEM((count, packed_rows, LANES), jnp.bfloat16),
            pltpu.VMEM((count, 1, LANES), jnp.float32),
        ],
        compiler_params=pltpu.CompilerParams(
            collective_id=0, has_side_effects=True, vmem_limit_bytes=56 * 1024 * 1024
        ),
    )(bins, leaf.reshape(chunks, LANES), grad, hess)
    gains = gains.reshape(owned, halves, LEAVES, LANES).transpose(0, 2, 1, 3).reshape(owned, LEAVES, B)
    return gains, best.reshape(LEAVES)


def solution(mesh):
    rows, feat = mesh.shape["rows"], mesh.shape["feat"]
    sizes = (rows // 2, 2, feat // 2)
    return jax.shard_map(
        functools.partial(shards, sizes),
        mesh=mesh,
        in_specs=(
            P(None, ("rows", "feat")),
            P(("rows", "feat")),
            P(None, ("rows", "feat")),
            P(None, ("rows", "feat")),
        ),
        out_specs=(P(("rows", "feat"), None, None), P()),
        check_vma=False,
    )
```
